32 devices in a mesh: seq: 8 (over z, y), head: 4 (over x, core).
Axes of the slice: x: 2, y: 2, z: 4, core: 2. Of those that a mesh axis runs over, the one named last changes fastest.
Arguments:
- inputs: bfloat16 [2048, 5120], P('seq', 'head'), may hold values from -6 to 6
- time_step: float32 [80, 2048], P('head', 'seq'), may hold values from 0.01 to 0.3
- decay_rate: float32 [80], P('head'), may hold values from 0.0001 to 1
- input_map: bfloat16 [2048, 128], P('seq'), may hold values from -6 to 6
- output_map: bfloat16 [2048, 128], P('seq'), may hold values from -0.59765625 to 0.59765625
- output_grad: bfloat16 [2048, 5120], P('seq', 'head'), may hold values from -3 to 3
- span_states: float32 [8, 80, 64, 128], P('seq', 'head'), may hold values from -6 to 6
- resets: int32 [8], P('seq'), may hold values from 0 to 4095
Outputs:
- grad_inputs: bfloat16 [2048, 5120], P('seq', 'head')
- grad_input_map: float32 [2048, 128], P('seq')
- grad_rate: float32 [80], P('head')
The draws below stay inside these ranges and needn't reach their ends.
Inputs may be any that keep to these rules, and one draw needn't show every extreme that they name: `resets`: A value p under 256 means that a document starts at position p of that span; a value of 256 or more means that none starts in it.
All inputs are finite; a program needn't handle non-finite values.
Results may differ from the reference program's by a relative error of at most 0.003.
Values sent between devices are 32-bit elements; how exact they have to be, the bound alone decides.
A program may use at most 64 MiB of HBM per device.

```python
import math
import jax
import jax.numpy as jnp
from jax import lax

NHEADS = 80
HEADDIM = 64
DSTATE = 128
SPAN = 256
TOKENS = 2048
NCHUNK = 8


def place_ends(array, stream_key, low, top_value):
    longest = array.shape.index(max(array.shape))
    spots = []
    for shift in (0, 1):
        where = [jax.random.randint(jax.random.fold_in(stream_key, axis), (), 0, length) for axis, length in enumerate(array.shape)]
        where[longest] = (where[longest] + shift) % array.shape[longest]
        spots.append(tuple(where))
    return array.at[spots[0]].set(low).at[spots[1]].set(top_value)


def steps_of(rng, dims, split, low, largest):
    factor_of = 1.0
    for dim, parts in split:
        heights = jax.random.uniform(jax.random.fold_in(jax.random.fold_in(rng, 6), dim), (parts,), jnp.float32, low / len(split), largest / len(split))
        factor_of = factor_of * jnp.repeat(jnp.exp(heights), dims[dim] // parts).reshape((-1,) + (1,) * (len(dims) - 1 - dim))
    return factor_of


def scatter_about(rng, extent, scale, bound, split=(), held_as=jnp.bfloat16):
    level = steps_of(rng, extent, split, -0.22, 0.18) if split else 1.0
    result = jax.random.normal(rng, extent, jnp.float32) * scale * level
    return jnp.minimum(jnp.maximum(result, -bound), bound).astype(held_as)


def setup_inputs(seed: int = 0) -> dict:
    streams_of = jax.random.split(jax.random.key(seed), 9)
    return {
        "inputs": scatter_about(streams_of[0], (TOKENS, NHEADS * HEADDIM), 1.0, 6.0, ((0, 8), (1, 4))),
        "time_step": jnp.clip(jnp.exp(math.log(0.3) - 3.4011974 * jax.random.uniform(streams_of[1], (NHEADS, TOKENS), jnp.float32) ** steps_of(streams_of[1], (NHEADS, TOKENS), ((0, 4), (1, 8)), -0.2, 0.2)), 0.01, 0.3),
        "decay_rate": jnp.clip(jnp.exp(math.log(1.0) - 9.2103404 * jax.random.uniform(streams_of[2], (NHEADS,), jnp.float32) ** steps_of(streams_of[2], (NHEADS,), ((0, 4),), -0.2, 0.2)), 0.0001, 1.0),
        "input_map": scatter_about(streams_of[3], (TOKENS, DSTATE), 1.0, 6.0, ((0, 8),)),
        "output_map": scatter_about(streams_of[4], (TOKENS, DSTATE), 0.1, 0.59765625, ((0, 8),)),
        "output_grad": scatter_about(streams_of[5], (TOKENS, NHEADS * HEADDIM), 0.5, 3.0, ((0, 8), (1, 4))),
        "span_states": scatter_about(streams_of[6], (NCHUNK, NHEADS, HEADDIM, DSTATE), 1.0, 6.0, ((0, 8), (1, 4)), jnp.float32),
        "resets": place_ends(jax.random.randint(streams_of[7], (NCHUNK,), 0, 16 * SPAN), jax.random.fold_in(streams_of[7], 1), 0, (16 * SPAN) - 1).astype(jnp.int32),
    }


highest = lax.Precision.HIGHEST


def prepare(x_block, step_block, decay_rate, b_block, c_block, grad_block, start_state, reset_at):
    block_len = step_block.shape[1]
    positions = jnp.arange(block_len, dtype=jnp.int32)
    later_doc = positions >= reset_at
    no_reset = reset_at >= block_len
    elapsed = jnp.cumsum(step_block, axis=1)
    log_decay = -decay_rate[:, None] * elapsed
    joined = (later_doc[:, None] == later_doc[None, :]) & (positions[None, :] >= positions[:, None])
    log_gaps = log_decay[:, None, :] - log_decay[:, :, None]
    pair_weight = jnp.where(joined[None], jnp.exp(jnp.where(joined[None], log_gaps, 0.0)), 0.0)
    intersection = jnp.dot(b_block, c_block.T, preferred_element_type=jnp.float32)
    products = jnp.einsum("shp,uhp->hsu", x_block.astype(jnp.float32), grad_block.astype(jnp.float32))
    mixing = (pair_weight * intersection[None]).astype(jnp.bfloat16)
    pair_terms = pair_weight * products
    paired = pair_terms.astype(jnp.bfloat16)
    dx_inner = jnp.einsum("hsu,uhp->shp", mixing.astype(jnp.float32), grad_block.astype(jnp.float32))
    db_inner = jnp.einsum("hsu,un->hsn", paired.astype(jnp.float32), c_block.astype(jnp.float32))
    start_weight = jnp.where(later_doc[None], 0.0, jnp.exp(log_decay))
    end_weight = jnp.where((later_doc | no_reset)[None], jnp.exp(log_decay[:, -1:] - log_decay), 0.0)
    carry_gain = jnp.where(no_reset, jnp.exp(log_decay[:, -1]), 0.0)
    c_wide = c_block.astype(jnp.float32)
    grad_wide = grad_block.astype(jnp.float32)
    weighted_c = start_weight[:, :, None] * c_wide[None]
    boundary_grad = jnp.einsum("hun,uhp->hpn", weighted_c, grad_wide, precision=highest)
    state_read = jnp.einsum("uhp,hpn->hun", grad_wide, start_state, precision=highest)
    start_term = jnp.sum(state_read * c_wide[None], axis=2)
    inside_term = jnp.sum(pair_terms * intersection[None] * step_block[:, :, None] * (elapsed[:, None, :] - elapsed[:, :, None]), axis=(1, 2))
    entry_term = jnp.sum(start_weight * elapsed * start_term, axis=1)
    return carry_gain, boundary_grad, dx_inner, db_inner, inside_term + entry_term, end_weight, elapsed


def finish(prepared, x_block, step_block, b_block, start_state, carried):
    carry_gain, boundary_grad, dx_inner, db_inner, partial_rate, end_weight, elapsed = prepared
    b_wide = b_block.astype(jnp.float32)
    x_wide = x_block.astype(jnp.float32)
    carried_b = jnp.einsum("sn,hpn->shp", b_wide, carried, precision=highest)
    carried_x = jnp.einsum("shp,hpn->hsn", x_wide, carried, precision=highest)
    step_rows = step_block.T[:, :, None]
    end_rows = end_weight.T[:, :, None]
    grad_x = (step_rows * (dx_inner + end_rows * carried_b)).astype(jnp.bfloat16)
    grad_b = jnp.sum(step_block[:, :, None] * (db_inner + end_weight[:, :, None] * carried_x), axis=0)
    last_elapsed = elapsed[:, -1]
    leaving_term = jnp.sum(end_weight * step_block * (last_elapsed[:, None] - elapsed) * jnp.sum(carried_x * b_wide[None], axis=2), axis=1)
    through_term = carry_gain * last_elapsed * jnp.sum(carried * start_state, axis=(1, 2))
    return grad_x, grad_b, partial_rate + leaving_term + through_term


def reference(inputs, time_step, decay_rate, input_map, output_map, output_grad, span_states, resets):
    x_all = inputs.reshape(NCHUNK, SPAN, NHEADS, HEADDIM)
    grad_all = output_grad.reshape(NCHUNK, SPAN, NHEADS, HEADDIM)
    step_all = time_step.reshape(NHEADS, NCHUNK, SPAN).transpose(1, 0, 2)
    b_all = input_map.reshape(NCHUNK, SPAN, DSTATE)
    c_all = output_map.reshape(NCHUNK, SPAN, DSTATE)

    def backward_block(carried, block_items):
        x_block, step_block, b_block, c_block, grad_block, start_state, reset_at = block_items
        prepared = prepare(x_block, step_block, decay_rate, b_block, c_block, grad_block, start_state, reset_at)
        grad_x, grad_b, rate_part = finish(prepared, x_block, step_block, b_block, start_state, carried)
        updated = prepared[1] + prepared[0][:, None, None] * carried
        return updated, (grad_x, grad_b, rate_part)

    initial = jnp.zeros((NHEADS, HEADDIM, DSTATE), jnp.float32)
    ending, outputs = lax.scan(backward_block, initial, (x_all, step_all, b_all, c_all, grad_all, span_states, resets.astype(jnp.int32)), reverse=True)
    grad_x_all, grad_b_all, rate_parts = outputs
    return (grad_x_all.reshape(TOKENS, NHEADS * HEADDIM), grad_b_all.reshape(TOKENS, DSTATE), -jnp.sum(rate_parts, axis=0))
```

```python
import functools

import jax
import jax.numpy as jnp
from jax import lax
from jax.experimental import pallas as pl
from jax.experimental.pallas import tpu as pltpu
from jax.sharding import PartitionSpec as P

MESH = pl.DeviceIdType.MESH
F32 = jnp.float32
BF16 = jnp.bfloat16
LANES = 128
LAG = 2


def split(value):
    high = value.astype(BF16)
    return high, (value - high.astype(F32)).astype(BF16)


def dot(a, b):
    return jnp.dot(a, b, preferred_element_type=F32)


def dot_nt(a, b):
    return lax.dot_general(a, b, (((1,), (1,)), ((), ())), preferred_element_type=F32)


def kernel(
    n, nh, width,
    x_ref, g_ref, dt_ref, dec_ref, b_ref, c_ref, s_ref, reset_ref,
    gx_ref, gb_ref, rate_ref,
    rows, ct, inter, acc, st, dxi, rate, bg, rxa, rxe, ebuf, ret, car,
    gbs, rxg, gsum, gfin, rtot, rxr,
    a_send, a_recv, e_send, e_recv, r_send, r_recv,
    g_send, g_recv, f_send, f_recv, t_send, t_recv,
):
    block_len = dt_ref.shape[1]
    head_count = dt_ref.shape[0]
    states = c_ref.shape[1]
    per = LANES // width
    chunks = head_count // per
    half = chunks // 2
    half_len = block_len // 2
    groups = n // 2
    me = lax.axis_index("seq")
    me_h = lax.axis_index("head")
    side = lax.rem(me, 2)
    group = lax.div(me, 2)
    partner = me + 1 - 2 * side
    below = jnp.maximum(me - 2, 0)
    last_group = group == groups - 1
    first_side = side == 0

    barrier = pltpu.get_barrier_semaphore()
    for d in range(1, n):
        pl.semaphore_signal(barrier, inc=1, device_id={"seq": lax.rem(me + d, n)}, device_id_type=MESH)
    for d in range(1, nh):
        pl.semaphore_signal(barrier, inc=1, device_id={"head": lax.rem(me_h + d, nh)}, device_id_type=MESH)

    reset_at = reset_ref[0]
    no_reset = reset_at >= block_len

    at_row = lax.broadcasted_iota(jnp.int32, (block_len, block_len), 0)
    at_col = lax.broadcasted_iota(jnp.int32, (block_len, block_len), 1)
    elapsed = jnp.dot(
        dt_ref[...], (at_row <= at_col).astype(F32),
        precision=lax.Precision.HIGHEST, preferred_element_type=F32,
    )
    for h in range(head_count):
        q, k = divmod(h, per)
        rows[q, k : k + 1, :] = elapsed[h : h + 1]
        rows[q, per + k : per + k + 1, :] = dt_ref[h : h + 1, :]
    ct[...] = c_ref[...].T
    joined = ((at_row >= reset_at) == (at_col >= reset_at)) & (at_col >= at_row)
    inter[...] = jnp.where(joined, dot_nt(b_ref[...], c_ref[...]), 0.0)
    acc[...] = jnp.zeros_like(acc)
    gbs[...] = jnp.zeros_like(gbs)

    @pl.when(last_group)
    def _():
        rxe[...] = jnp.zeros_like(rxe)

    lane_of = lax.broadcasted_iota(jnp.int32, (1, LANES), 1)

    def spread(items):
        out = items[0]
        for k in range(1, per):
            out = jnp.where(lane_of >= k * width, items[k], out)
        return out

    def columns(j):
        return rows[j].T

    def at(j):
        return pl.ds(pl.multiple_of(j * LANES, LANES), LANES)

    def lanes(cols, kind):
        return spread([cols[:, kind * per + k : kind * per + k + 1] for k in range(per)])

    def copy_a(jj):
        return pltpu.make_async_remote_copy(
            src_ref=bg.at[(1 - side) * half + jj], dst_ref=rxa.at[jj],
            send_sem=a_send.at[jj], recv_sem=a_recv.at[jj],
            device_id={"seq": partner}, device_id_type=MESH,
        )

    def copy_e(jj):
        return pltpu.make_async_remote_copy(
            src_ref=ebuf.at[jj], dst_ref=rxe.at[jj],
            send_sem=e_send.at[jj], recv_sem=e_recv.at[jj],
            device_id={"seq": below}, device_id_type=MESH,
        )

    def copy_r(jj):
        return pltpu.make_async_remote_copy(
            src_ref=ret.at[jj], dst_ref=car.at[side * half + jj],
            send_sem=r_send.at[jj], recv_sem=r_recv.at[jj],
            device_id={"seq": partner}, device_id_type=MESH,
        )

    def boundary(j):
        now = rows[j]
        row_of = lax.broadcasted_iota(jnp.int32, (per, block_len), 0)
        token = lax.broadcasted_iota(jnp.int32, (per, block_len), 1)
        later = token >= reset_at
        decay = jnp.full((per, block_len), dec_ref[j * per], F32)
        for k in range(1, per):
            decay = jnp.where(row_of == k, dec_ref[j * per + k], decay)
        log_decay = -decay * now[0:per]
        final = log_decay[:, block_len - 1 : block_len]
        rows[j, 2 * per : 3 * per, :] = jnp.where(later, 0.0, jnp.exp(log_decay))
        rows[j, 3 * per : 4 * per, :] = jnp.where(later | no_reset, jnp.exp(final - log_decay), 0.0)
        gain = jnp.where(no_reset, jnp.exp(final), 0.0)
        cols = columns(j)
        weighted = g_ref[:, at(j)].astype(F32) * lanes(cols, 2)
        high, low = split(weighted)
        bg[j, 0:states, :] = dot(ct[...], high) + dot(ct[...], low)
        gain_row = spread([gain[k : k + 1, :] for k in range(per)])
        bg[j, states : states + 8, :] = jnp.broadcast_to(gain_row, (8, LANES))

    boundary((1 - side) * half)
    pl.semaphore_wait(barrier, n + nh - 2)

    def give(jj, _):
        boundary((1 - side) * half + jj)
        copy_a(jj - 1).start()
        return 0

    lax.fori_loop(1, half, give, 0)
    boundary(side * half)
    copy_a(half - 1).start()

    def keep(jj, _):
        boundary(side * half + jj)
        return 0

    lax.fori_loop(1, half, keep, 0)

    def relay(jj):
        j = side * half + jj
        copy_a(jj).wait_recv()

        @pl.when(jnp.logical_not(last_group))
        def _():
            copy_e(jj).wait_recv()

        own = bg[j]
        other = rxa[jj]
        early = jnp.where(first_side, own, other)
        late = jnp.where(first_side, other, own)
        ending = rxe[jj]
        first = late[0:states] + late[states : states + 1] * ending

        @pl.when(group > 0)
        def _():
            ebuf[jj] = early[0:states] + early[states : states + 1] * first

        car[j] = jnp.where(first_side, first, ending)
        ret[jj] = jnp.where(first_side, ending, first)

        @pl.when(group > 0)
        def _():
            copy_e(jj).start()

        copy_r(jj).start()

    def pairs(j):
        now = rows[j]
        cols = columns(j)
        x_two = x_ref[:, at(j)]
        g_two = g_ref[:, at(j)]
        low_g = g_two[half_len:]
        inner = []
        terms = []
        for k in range(per):
            mine = (lane_of >= k * width) & (lane_of < (k + 1) * width)
            x_one = jnp.where(mine, x_two, jnp.zeros_like(x_two))
            rate_of = -dec_ref[j * per + k]
            parts = []
            total = jnp.zeros((1, LANES), F32)
            for top, left in ((0, 0), (half_len, half_len)):
                s_of = slice(top, top + half_len)
                u_of = slice(left, block_len)
                grad = g_two if left == 0 else low_g
                products = dot_nt(x_one[s_of], grad)
                gaps = now[k : k + 1, u_of] - cols[s_of, k : k + 1]
                gaps = jnp.maximum(gaps, 0.0)
                weight = jnp.exp(gaps * rate_of)
                mixing = weight * inter[s_of, u_of]
                scaled = weight * products * cols[s_of, per + k : per + k + 1]
                acc[s_of, u_of] += scaled
                parts.append(dot(mixing.astype(BF16), grad))
                inside = jnp.sum(mixing * gaps * products * cols[s_of, per + k : per + k + 1], axis=0, keepdims=True)
                for piece in range(0, inside.shape[1], LANES):
                    total = total + inside[:, piece : piece + LANES]
            inner.append(jnp.concatenate(parts, axis=0))
            shifted = total
            for k2 in range(1, per):
                shifted = shifted + pltpu.roll(total, k2 * width, 1)
            terms.append(shifted)
        dxi[j] = spread(inner)
        inside_row = spread(terms)
        state = s_ref[pl.ds(j * per, per)].reshape(LANES, states).T
        st[j] = state
        high, low = split(state)
        read = dot(c_ref[...], high) + dot(c_ref[...], low)
        entry = g_two.astype(F32) * read * (lanes(cols, 2) * lanes(cols, 0))
        entry_row = jnp.sum(entry, axis=0, keepdims=True)
        rate[j] = jnp.broadcast_to(inside_row + entry_row, (8, LANES))

    lag = (groups - 1 - group) * LAG

    def slot(t, _):
        jj = t - lag

        @pl.when((jj >= 0) & (jj < half))
        def _():
            relay(jj)

        @pl.when(t < chunks)
        def _():
            pairs(t)

        return 0

    lax.fori_loop(0, max(chunks, half + (groups - 1) * LAG), slot, 0)

    def finish(j):
        cols = columns(j)
        carried = car[j]
        high, low = split(carried)
        through = jnp.sum(carried * st[j], axis=0, keepdims=True)
        step = lanes(cols, 1)
        end = lanes(cols, 3)
        spent = lanes(cols, 0)
        last = spent[block_len - 1 : block_len]
        reach = end * (dot(b_ref[...], high) + dot(b_ref[...], low))
        gx_ref[:, at(j)] = (step * (dxi[j] + reach)).astype(BF16)
        x_step = x_ref[:, at(j)].astype(F32) * step
        leaving = jnp.sum(x_step * reach * (last - spent), axis=0, keepdims=True)
        x_high, x_low = split(x_step * end)
        gbs[...] += dot_nt(x_high, high) + dot_nt(x_high, low) + dot_nt(x_low, high)
        gain_row = bg[j, states : states + 1, :]
        rate[j] += jnp.broadcast_to(leaving + gain_row * last * through, (8, LANES))

    def closing(jj, _):
        finish(side * half + jj)
        pltpu.make_async_remote_copy(
            src_ref=ret.at[jj], dst_ref=car.at[(1 - side) * half + jj],
            send_sem=r_send.at[jj], recv_sem=r_recv.at[jj],
            device_id={"seq": partner}, device_id_type=MESH,
        ).wait_recv()
        finish((1 - side) * half + jj)
        return 0

    summed = jnp.where(joined, acc[...], 0.0)
    sum_high, sum_low = split(summed)
    gbs[...] += dot(sum_high, c_ref[...]) + dot(sum_low, c_ref[...])
    lax.fori_loop(0, half, closing, 0)

    share = block_len // nh

    def copy_g(d):
        peer = lax.rem(me_h + d, nh)
        return pltpu.make_async_remote_copy(
            src_ref=gbs.at[pl.ds(pl.multiple_of(peer * share, share), share)], dst_ref=rxg.at[d],
            send_sem=g_send.at[d], recv_sem=g_recv.at[d],
            device_id={"head": peer}, device_id_type=MESH,
        )

    def copy_f(d):
        peer = lax.rem(me_h + d, nh)
        return pltpu.make_async_remote_copy(
            src_ref=gsum, dst_ref=gfin.at[d],
            send_sem=f_send.at[d], recv_sem=f_recv.at[d],
            device_id={"head": peer}, device_id_type=MESH,
        )

    def copy_t(d):
        return pltpu.make_async_remote_copy(
            src_ref=rtot, dst_ref=rxr.at[d],
            send_sem=t_send.at[d], recv_sem=t_recv.at[d],
            device_id={"seq": lax.rem(me + d, n)}, device_id_type=MESH,
        )

    for d in range(1, nh):
        copy_g(d).start()

    parity = lax.broadcasted_iota(jnp.int32, (LANES, LANES), 0) // width
    target = lax.broadcasted_iota(jnp.int32, (LANES, LANES), 1)
    chosen = (lax.rem(target, per) == parity).astype(F32)
    folded = jnp.concatenate([rate[j, 0:1, :] for j in range(chunks)], axis=0)
    sums = jnp.dot(folded, chosen, precision=lax.Precision.HIGHEST, preferred_element_type=F32)
    home = lax.broadcasted_iota(jnp.int32, (chunks, LANES), 1) // per
    which = lax.broadcasted_iota(jnp.int32, (chunks, LANES), 0)
    mine_rate = jnp.sum(jnp.where(home == which, sums, 0.0), axis=0, keepdims=True)
    rtot[...] = jnp.broadcast_to(mine_rate, (8, LANES))

    own_share = gbs[pl.ds(pl.multiple_of(me_h * share, share), share), :]
    for d in range(1, n):
        copy_t(d).start()
    for d in range(1, nh):
        copy_g(d).wait_recv()
        own_share = own_share + rxg[d]
    gsum[...] = own_share
    gb_ref[pl.ds(pl.multiple_of(me_h * share, share), share), :] = own_share
    for d in range(1, nh):
        copy_f(d).start()
    all_rate = rtot[...]
    for d in range(1, n):
        copy_t(d).wait_recv()
        all_rate = all_rate + rxr[d]
    rate_ref[...] = -all_rate
    for d in range(1, nh):
        copy_f(d).wait_recv()
        source = lax.rem(me_h + nh - d, nh)
        gb_ref[pl.ds(pl.multiple_of(source * share, share), share), :] = gfin[d]

    for jj in range(half):
        copy_a(jj).wait_send()
        copy_r(jj).wait_send()

    @pl.when(group > 0)
    def _():
        for jj in range(half):
            copy_e(jj).wait_send()

    for d in range(1, nh):
        copy_g(d).wait_send()
        copy_f(d).wait_send()
    for d in range(1, n):
        copy_t(d).wait_send()


def body(n, nh, inputs, time_step, decay_rate, input_map, output_map, output_grad, span_states, resets):
    head_count, block_len = time_step.shape
    width, states = span_states.shape[2:]
    chunks = inputs.shape[1] // LANES
    half = chunks // 2
    share = block_len // nh
    vmem = pl.BlockSpec(memory_space=pltpu.VMEM)
    smem = pl.BlockSpec(memory_space=pltpu.SMEM)
    sem = pltpu.SemaphoreType.DMA
    grad_inputs, grad_map, rates = pl.pallas_call(
        functools.partial(kernel, n, nh, width),
        out_shape=(
            jax.ShapeDtypeStruct(inputs.shape, BF16),
            jax.ShapeDtypeStruct((block_len, states), F32),
            jax.ShapeDtypeStruct((8, LANES), F32),
        ),
        in_specs=[vmem, vmem, vmem, smem, vmem, vmem, vmem, smem],
        out_specs=(vmem, vmem, vmem),
        scratch_shapes=[
            pltpu.VMEM((chunks, 8, block_len), F32),
            pltpu.VMEM((states, block_len), BF16),
            pltpu.VMEM((block_len, block_len), F32),
            pltpu.VMEM((block_len, block_len), F32),
            pltpu.VMEM((chunks, states, LANES), F32),
            pltpu.VMEM((chunks, block_len, LANES), F32),
            pltpu.VMEM((chunks, 8, LANES), F32),
            pltpu.VMEM((chunks, states + 8, LANES), F32),
            pltpu.VMEM((half, states + 8, LANES), F32),
            pltpu.VMEM((half, states, LANES), F32),
            pltpu.VMEM((half, states, LANES), F32),
            pltpu.VMEM((half, states, LANES), F32),
            pltpu.VMEM((chunks, states, LANES), F32),
            pltpu.VMEM((block_len, states), F32),
            pltpu.VMEM((nh, share, states), F32),
            pltpu.VMEM((share, states), F32),
            pltpu.VMEM((nh, share, states), F32),
            pltpu.VMEM((8, LANES), F32),
            pltpu.VMEM((n, 8, LANES), F32),
            sem((half,)), sem((half,)), sem((half,)), sem((half,)), sem((half,)), sem((half,)),
            sem((nh,)), sem((nh,)), sem((nh,)), sem((nh,)), sem((n,)), sem((n,)),
        ],
        compiler_params=pltpu.CompilerParams(
            collective_id=0, has_side_effects=True, vmem_limit_bytes=48 * 2**20
        ),
    )(inputs, output_grad, time_step, decay_rate, input_map, output_map, span_states[0], resets)
    return grad_inputs, grad_map, rates[0, :head_count]


def solution(mesh):
    in_specs = (
        P("seq", "head"),
        P("head", "seq"),
        P("head"),
        P("seq", None),
        P("seq", None),
        P("seq", "head"),
        P("seq", "head", None, None),
        P("seq"),
    )
    out_specs = (P("seq", "head"), P("seq", None), P("head"))
    run = functools.partial(body, mesh.shape["seq"], mesh.shape["head"])
    return jax.shard_map(run, mesh=mesh, in_specs=in_specs, out_specs=out_specs, check_vma=False)
```

```python
import functools

import jax
import jax.numpy as jnp
from jax import lax
from jax.experimental import pallas as pl
from jax.experimental.pallas import tpu as pltpu
from jax.sharding import PartitionSpec as P

MESH = pl.DeviceIdType.MESH
F32 = jnp.float32
BF16 = jnp.bfloat16
LANES = 128
LAG = 3
GAIN_ROWS = 8
PIECES = 2


def split(value):
    high = value.astype(BF16)
    return high, (value - high.astype(F32)).astype(BF16)


def dot(a, b):
    return jnp.dot(a, b, preferred_element_type=F32)


def dot_nt(a, b):
    return lax.dot_general(a, b, (((1,), (1,)), ((), ())), preferred_element_type=F32)


def kernel(
    n, nh, width,
    x_in, g_in, dt_in, dec_in, b_in, c_in, s_in, reset_in,
    gx_ref, gb_ref, rate_ref,
    x_ref, g_ref, dt_ref, dec_ref, b_ref, c_ref, s_ref, reset_ref, in_sem,
    rows, ct, inter, acc, st, dxi, rate, bg, rxa, rxe, ebuf, ret, car,
    gbs, rxg, gsum, gfin, rtot, rxr,
    a_send, a_recv, e_send, e_recv, r_send, r_recv,
    g_send, g_recv, f_send, f_recv, t_send, t_recv,
):
    loads = {}
    names = ("dt", "dec", "reset", "c", "g", "b", "x", "s")
    places = ((dt_in, dt_ref), (dec_in, dec_ref), (reset_in, reset_ref), (c_in, c_ref),
              (g_in, g_ref), (b_in, b_ref), (x_in, x_ref), (s_in, s_ref))
    for number, (source, target) in enumerate(places):
        loads[names[number]] = pltpu.make_async_copy(source, target, in_sem.at[number])
        loads[names[number]].start()
    block_len = dt_ref.shape[1]
    head_count = dt_ref.shape[0]
    states = c_ref.shape[1]
    per = LANES // width
    chunks = head_count // per
    half = chunks // 2
    half_len = block_len // 2
    groups = n // 2
    me = lax.axis_index("seq")
    me_h = lax.axis_index("head")
    side = lax.rem(me, 2)
    group = lax.div(me, 2)
    partner = me + 1 - 2 * side
    below = jnp.maximum(me - 2, 0)
    last_group = group == groups - 1
    first_side = side == 0

    barrier = pltpu.get_barrier_semaphore()
    for d in range(1, n):
        pl.semaphore_signal(barrier, inc=1, device_id={"seq": lax.rem(me + d, n)}, device_id_type=MESH)
    for d in range(1, nh):
        pl.semaphore_signal(barrier, inc=1, device_id={"head": lax.rem(me_h + d, nh)}, device_id_type=MESH)

    loads["dec"].wait()
    loads["reset"].wait()
    reset_at = reset_ref[0]
    no_reset = reset_at >= block_len

    at_row = lax.broadcasted_iota(jnp.int32, (block_len, block_len), 0)
    at_col = lax.broadcasted_iota(jnp.int32, (block_len, block_len), 1)
    loads["dt"].wait()
    elapsed = jnp.dot(
        dt_ref[...], (at_row <= at_col).astype(F32),
        precision=lax.Precision.HIGHEST, preferred_element_type=F32,
    )
    for h in range(head_count):
        q, k = divmod(h, per)
        rows[q, k : k + 1, :] = elapsed[h : h + 1]
        rows[q, per + k : per + k + 1, :] = dt_ref[h : h + 1, :]
    loads["c"].wait()
    ct[...] = c_ref[...].T
    lane_of = lax.broadcasted_iota(jnp.int32, (1, LANES), 1)

    def spread(items):
        out = items[0]
        for k in range(1, per):
            out = jnp.where(lane_of >= k * width, items[k], out)
        return out

    def columns(j):
        return rows[j].T

    def at(j):
        return pl.ds(pl.multiple_of(j * LANES, LANES), LANES)

    def lanes(cols, kind):
        return spread([cols[:, kind * per + k : kind * per + k + 1] for k in range(per)])

    part = states // PIECES

    def span(p):
        begin = GAIN_ROWS + p * part if p else 0
        return pl.ds(begin, GAIN_ROWS + (p + 1) * part - begin)

    def of(p):
        return pl.ds(p * part, part)

    def copy_a(jj, p):
        return pltpu.make_async_remote_copy(
            src_ref=bg.at[(1 - side) * half + jj, span(p)], dst_ref=rxa.at[jj, span(p)],
            send_sem=a_send.at[jj, p], recv_sem=a_recv.at[jj, p],
            device_id={"seq": partner}, device_id_type=MESH,
        )

    def copy_e(jj, p):
        return pltpu.make_async_remote_copy(
            src_ref=ebuf.at[jj, of(p)], dst_ref=rxe.at[jj, of(p)],
            send_sem=e_send.at[jj, p], recv_sem=e_recv.at[jj, p],
            device_id={"seq": below}, device_id_type=MESH,
        )

    def copy_r(jj, p, holder):
        return pltpu.make_async_remote_copy(
            src_ref=ret.at[jj, of(p)], dst_ref=car.at[holder * half + jj, of(p)],
            send_sem=r_send.at[jj, p], recv_sem=r_recv.at[jj, p],
            device_id={"seq": partner}, device_id_type=MESH,
        )

    def boundary(j):
        now = rows[j]
        row_of = lax.broadcasted_iota(jnp.int32, (per, block_len), 0)
        token = lax.broadcasted_iota(jnp.int32, (per, block_len), 1)
        later = token >= reset_at
        decay = jnp.full((per, block_len), dec_ref[j * per], F32)
        for k in range(1, per):
            decay = jnp.where(row_of == k, dec_ref[j * per + k], decay)
        log_decay = -decay * now[0:per]
        final = log_decay[:, block_len - 1 : block_len]
        rows[j, 2 * per : 3 * per, :] = jnp.where(later, 0.0, jnp.exp(log_decay))
        rows[j, 3 * per : 4 * per, :] = jnp.where(later | no_reset, jnp.exp(final - log_decay), 0.0)
        gain = jnp.where(no_reset, jnp.exp(final), 0.0)
        cols = columns(j)
        weighted = g_ref[:, at(j)].astype(F32) * lanes(cols, 2)
        high, low = split(weighted)
        bg[j, GAIN_ROWS : GAIN_ROWS + states, :] = dot(ct[...], high) + dot(ct[...], low)
        gain_row = spread([gain[k : k + 1, :] for k in range(per)])
        bg[j, 0:GAIN_ROWS, :] = jnp.broadcast_to(gain_row, (GAIN_ROWS, LANES))

    loads["g"].wait()
    boundary((1 - side) * half)
    pl.semaphore_wait(barrier, n + nh - 2)

    def give(jj, _):
        boundary((1 - side) * half + jj)
        for p in range(PIECES):
            copy_a(jj - 1, p).start()
        return 0

    lax.fori_loop(1, half, give, 0)
    boundary(side * half)
    for p in range(PIECES):
        copy_a(half - 1, p).start()

    def keep(jj, _):
        boundary(side * half + jj)
        return 0

    lax.fori_loop(1, half, keep, 0)

    loads["b"].wait()
    joined = ((at_row >= reset_at) == (at_col >= reset_at)) & (at_col >= at_row)
    inter[...] = jnp.where(joined, dot_nt(b_ref[...], c_ref[...]), 0.0)
    acc[...] = jnp.zeros_like(acc)
    gbs[...] = jnp.zeros_like(gbs)

    @pl.when(last_group)
    def _():
        rxe[...] = jnp.zeros_like(rxe)

    loads["x"].wait()
    loads["s"].wait()

    def relay(jj):
        j = side * half + jj
        for p in range(PIECES):
            copy_a(jj, p).wait_recv()

            @pl.when(jnp.logical_not(last_group))
            def _():
                copy_e(jj, p).wait_recv()

            if p == 0:
                own_gain = bg[j, 0:1, :]
                other_gain = rxa[jj, 0:1, :]
                early_gain = jnp.where(first_side, own_gain, other_gain)
                late_gain = jnp.where(first_side, other_gain, own_gain)
            here = pl.ds(GAIN_ROWS + p * part, part)
            own = bg[j, here, :]
            other = rxa[jj, here, :]
            early = jnp.where(first_side, own, other)
            late = jnp.where(first_side, other, own)
            ending = rxe[jj, of(p), :]
            first = late + late_gain * ending

            @pl.when(group > 0)
            def _():
                ebuf[jj, of(p), :] = early + early_gain * first

            car[j, of(p), :] = jnp.where(first_side, first, ending)
            ret[jj, of(p), :] = jnp.where(first_side, ending, first)

            @pl.when(group > 0)
            def _():
                copy_e(jj, p).start()

            copy_r(jj, p, side).start()

    def pairs(j):
        now = rows[j]
        cols = columns(j)
        x_two = x_ref[:, at(j)]
        g_two = g_ref[:, at(j)]
        low_g = g_two[half_len:]
        inner = []
        terms = []
        for k in range(per):
            mine = (lane_of >= k * width) & (lane_of < (k + 1) * width)
            x_one = jnp.where(mine, x_two, jnp.zeros_like(x_two))
            rate_of = -dec_ref[j * per + k]
            parts = []
            total = jnp.zeros((1, LANES), F32)
            for top, left in ((0, 0), (half_len, half_len)):
                s_of = slice(top, top + half_len)
                u_of = slice(left, block_len)
                grad = g_two if left == 0 else low_g
                products = dot_nt(x_one[s_of], grad)
                gaps = now[k : k + 1, u_of] - cols[s_of, k : k + 1]
                gaps = jnp.maximum(gaps, 0.0)
                weight = jnp.exp(gaps * rate_of)
                mixing = weight * inter[s_of, u_of]
                scaled = weight * products * cols[s_of, per + k : per + k + 1]
                acc[s_of, u_of] += scaled
                parts.append(dot(mixing.astype(BF16), grad))
                inside = jnp.sum(mixing * gaps * products * cols[s_of, per + k : per + k + 1], axis=0, keepdims=True)
                for piece in range(0, inside.shape[1], LANES):
                    total = total + inside[:, piece : piece + LANES]
            inner.append(jnp.concatenate(parts, axis=0))
            shifted = total
            for k2 in range(1, per):
                shifted = shifted + pltpu.roll(total, k2 * width, 1)
            terms.append(shifted)
        dxi[j] = spread(inner)
        inside_row = spread(terms)
        state = s_ref[pl.ds(j * per, per)].reshape(LANES, states).T
        st[j] = state
        high, low = split(state)
        read = dot(c_ref[...], high) + dot(c_ref[...], low)
        entry = g_two.astype(F32) * read * (lanes(cols, 2) * lanes(cols, 0))
        entry_row = jnp.sum(entry, axis=0, keepdims=True)
        rate[j] = jnp.broadcast_to(inside_row + entry_row, (8, LANES))

    def finish(j):
        cols = columns(j)
        carried = car[j]
        high, low = split(carried)
        through = jnp.sum(carried * st[j], axis=0, keepdims=True)
        step = lanes(cols, 1)
        end = lanes(cols, 3)
        spent = lanes(cols, 0)
        last = spent[block_len - 1 : block_len]
        reach = end * (dot(b_ref[...], high) + dot(b_ref[...], low))
        gx_ref[:, at(j)] = (step * (dxi[j] + reach)).astype(BF16)
        x_step = x_ref[:, at(j)].astype(F32) * step
        leaving = jnp.sum(x_step * reach * (last - spent), axis=0, keepdims=True)
        x_high, x_low = split(x_step * end)
        gbs[...] += dot_nt(x_high, high) + dot_nt(x_high, low) + dot_nt(x_low, high)
        gain_row = bg[j, 0:1, :]
        rate[j] += jnp.broadcast_to(leaving + gain_row * last * through, (8, LANES))

    base = max(chunks - 1, (groups - 1) * LAG)
    lag = base - group * LAG

    def slot(t, _):
        jj = t - lag

        @pl.when((jj >= 0) & (jj < half))
        def _():
            relay(jj)

        @pl.when(t < chunks)
        def _():
            pairs(t)

        @pl.when((t >= base) & (t < base + half))
        def _():
            finish(side * half + t - base)

        late = t - base - 2

        @pl.when(late >= 0)
        def _():
            for p in range(PIECES):
                copy_r(late, p, 1 - side).wait_recv()
            finish((1 - side) * half + late)

        return 0

    lax.fori_loop(0, base + half, slot, 0)
    summed = jnp.where(joined, acc[...], 0.0)
    sum_high, sum_low = split(summed)
    gbs[...] += dot(sum_high, c_ref[...]) + dot(sum_low, c_ref[...])
    lax.fori_loop(base + half, base + half + 2, slot, 0)

    share = block_len // nh

    def copy_g(d):
        peer = lax.rem(me_h + d, nh)
        return pltpu.make_async_remote_copy(
            src_ref=gbs.at[pl.ds(pl.multiple_of(peer * share, share), share)], dst_ref=rxg.at[d],
            send_sem=g_send.at[d], recv_sem=g_recv.at[d],
            device_id={"head": peer}, device_id_type=MESH,
        )

    def copy_f(d):
        peer = lax.rem(me_h + d, nh)
        return pltpu.make_async_remote_copy(
            src_ref=gsum, dst_ref=gfin.at[d],
            send_sem=f_send.at[d], recv_sem=f_recv.at[d],
            device_id={"head": peer}, device_id_type=MESH,
        )

    def copy_t(d):
        return pltpu.make_async_remote_copy(
            src_ref=rtot, dst_ref=rxr.at[d],
            send_sem=t_send.at[d], recv_sem=t_recv.at[d],
            device_id={"seq": lax.rem(me + d, n)}, device_id_type=MESH,
        )

    for d in range(1, nh):
        copy_g(d).start()

    parity = lax.broadcasted_iota(jnp.int32, (LANES, LANES), 0) // width
    target = lax.broadcasted_iota(jnp.int32, (LANES, LANES), 1)
    chosen = (lax.rem(target, per) == parity).astype(F32)
    folded = jnp.concatenate([rate[j, 0:1, :] for j in range(chunks)], axis=0)
    sums = jnp.dot(folded, chosen, precision=lax.Precision.HIGHEST, preferred_element_type=F32)
    home = lax.broadcasted_iota(jnp.int32, (chunks, LANES), 1) // per
    which = lax.broadcasted_iota(jnp.int32, (chunks, LANES), 0)
    mine_rate = jnp.sum(jnp.where(home == which, sums, 0.0), axis=0, keepdims=True)
    rtot[...] = jnp.broadcast_to(mine_rate, (8, LANES))

    own_share = gbs[pl.ds(pl.multiple_of(me_h * share, share), share), :]
    for d in range(1, n):
        copy_t(d).start()
    for d in range(1, nh):
        copy_g(d).wait_recv()
        own_share = own_share + rxg[d]
    gsum[...] = own_share
    gb_ref[pl.ds(pl.multiple_of(me_h * share, share), share), :] = own_share
    for d in range(1, nh):
        copy_f(d).start()
    all_rate = rtot[...]
    for d in range(1, n):
        copy_t(d).wait_recv()
        all_rate = all_rate + rxr[d]
    rate_ref[...] = -all_rate
    for d in range(1, nh):
        copy_f(d).wait_recv()
        source = lax.rem(me_h + nh - d, nh)
        gb_ref[pl.ds(pl.multiple_of(source * share, share), share), :] = gfin[d]

    for jj in range(half):
        for p in range(PIECES):
            copy_a(jj, p).wait_send()
            copy_r(jj, p, side).wait_send()

    @pl.when(group > 0)
    def _():
        for jj in range(half):
            for p in range(PIECES):
                copy_e(jj, p).wait_send()

    for d in range(1, nh):
        copy_g(d).wait_send()
        copy_f(d).wait_send()
    for d in range(1, n):
        copy_t(d).wait_send()


def body(n, nh, inputs, time_step, decay_rate, input_map, output_map, output_grad, span_states, resets):
    head_count, block_len = time_step.shape
    width, states = span_states.shape[2:]
    chunks = inputs.shape[1] // LANES
    half = chunks // 2
    share = block_len // nh
    vmem = pl.BlockSpec(memory_space=pltpu.VMEM)
    hbm = pl.BlockSpec(memory_space=pltpu.HBM)
    sem = pltpu.SemaphoreType.DMA
    grad_inputs, grad_map, rates = pl.pallas_call(
        functools.partial(kernel, n, nh, width),
        out_shape=(
            jax.ShapeDtypeStruct(inputs.shape, BF16),
            jax.ShapeDtypeStruct((block_len, states), F32),
            jax.ShapeDtypeStruct((8, LANES), F32),
        ),
        in_specs=[hbm] * 8,
        out_specs=(vmem, vmem, vmem),
        scratch_shapes=[
            pltpu.VMEM(inputs.shape, BF16),
            pltpu.VMEM(inputs.shape, BF16),
            pltpu.VMEM(time_step.shape, F32),
            pltpu.SMEM(decay_rate.shape, F32),
            pltpu.VMEM(input_map.shape, BF16),
            pltpu.VMEM(output_map.shape, BF16),
            pltpu.VMEM(span_states.shape[1:], F32),
            pltpu.SMEM(resets.shape, jnp.int32),
            sem((8,)),
            pltpu.VMEM((chunks, 8, block_len), F32),
            pltpu.VMEM((states, block_len), BF16),
            pltpu.VMEM((block_len, block_len), F32),
            pltpu.VMEM((block_len, block_len), F32),
            pltpu.VMEM((chunks, states, LANES), F32),
            pltpu.VMEM((chunks, block_len, LANES), F32),
            pltpu.VMEM((chunks, 8, LANES), F32),
            pltpu.VMEM((chunks, states + GAIN_ROWS, LANES), F32),
            pltpu.VMEM((half, states + GAIN_ROWS, LANES), F32),
            pltpu.VMEM((half, states, LANES), F32),
            pltpu.VMEM((half, states, LANES), F32),
            pltpu.VMEM((half, states, LANES), F32),
            pltpu.VMEM((chunks, states, LANES), F32),
            pltpu.VMEM((block_len, states), F32),
            pltpu.VMEM((nh, share, states), F32),
            pltpu.VMEM((share, states), F32),
            pltpu.VMEM((nh, share, states), F32),
            pltpu.VMEM((8, LANES), F32),
            pltpu.VMEM((n, 8, LANES), F32),
            *[sem((half, PIECES)) for _ in range(6)],
            sem((nh,)), sem((nh,)), sem((nh,)), sem((nh,)), sem((n,)), sem((n,)),
        ],
        compiler_params=pltpu.CompilerParams(
            collective_id=0, has_side_effects=True, vmem_limit_bytes=40 * 2**20
        ),
    )(inputs, output_grad, time_step, decay_rate, input_map, output_map, span_states.reshape(span_states.shape[1:]), resets)
    return grad_inputs, grad_map, rates[0, :head_count]


def solution(mesh):
    in_specs = (
        P("seq", "head"),
        P("head", "seq"),
        P("head"),
        P("seq", None),
        P("seq", None),
        P("seq", "head"),
        P("seq", "head", None, None),
        P("seq"),
    )
    out_specs = (P("seq", "head"), P("seq", None), P("head"))
    run = functools.partial(body, mesh.shape["seq"], mesh.shape["head"])
    return jax.shard_map(run, mesh=mesh, in_specs=in_specs, out_specs=out_specs, check_vma=False)
```

```python
import functools

import jax
import jax.numpy as jnp
from jax import lax
from jax.experimental import pallas as pl
from jax.experimental.pallas import tpu as pltpu
from jax.sharding import PartitionSpec as P

MESH = pl.DeviceIdType.MESH
F32 = jnp.float32
BF16 = jnp.bfloat16
LANES = 128
LAG = 3
GAIN_ROWS = 8
PIECES = 2


def split(value):
    high = value.astype(BF16)
    return high, (value - high.astype(F32)).astype(BF16)


def dot(a, b):
    return jnp.dot(a, b, preferred_element_type=F32)


def dot_nt(a, b):
    return lax.dot_general(a, b, (((1,), (1,)), ((), ())), preferred_element_type=F32)


def kernel(
    n, nh, width,
    x_in, g_in, dt_in, dec_in, b_in, c_in, s_in, reset_in,
    gx_ref, gb_ref, rate_ref,
    x_ref, g_ref, dt_ref, dec_ref, b_ref, c_ref, s_ref, reset_ref, in_sem,
    rows, ct, inter, acc, st, dxi, rate, bg, rxa, rxe, ebuf, ret, car,
    gbs, rxg, gsum, gfin, rtot, rxr,
    a_send, a_recv, e_send, e_recv, r_send, r_recv,
    g_send, g_recv, f_send, f_recv, t_send, t_recv,
):
    loads = {}
    names = ("dt", "dec", "reset", "c", "g", "b", "x", "s")
    places = ((dt_in, dt_ref), (dec_in, dec_ref), (reset_in, reset_ref), (c_in, c_ref),
              (g_in, g_ref), (b_in, b_ref), (x_in, x_ref), (s_in, s_ref))
    for number, (source, target) in enumerate(places):
        loads[names[number]] = pltpu.make_async_copy(source, target, in_sem.at[number])
        loads[names[number]].start()
    block_len = dt_ref.shape[1]
    head_count = dt_ref.shape[0]
    states = c_ref.shape[1]
    per = LANES // width
    chunks = head_count // per
    half = chunks // 2
    half_len = block_len // 2
    groups = n // 2
    me = lax.axis_index("seq")
    me_h = lax.axis_index("head")
    side = lax.rem(me, 2)
    group = lax.div(me, 2)
    partner = me + 1 - 2 * side
    below = jnp.maximum(me - 2, 0)
    last_group = group == groups - 1
    first_side = side == 0

    barrier = pltpu.get_barrier_semaphore()
    for d in range(1, n):
        pl.semaphore_signal(barrier, inc=1, device_id={"seq": lax.rem(me + d, n)}, device_id_type=MESH)
    for d in range(1, nh):
        pl.semaphore_signal(barrier, inc=1, device_id={"head": lax.rem(me_h + d, nh)}, device_id_type=MESH)

    loads["dec"].wait()
    loads["reset"].wait()
    reset_at = reset_ref[0]
    no_reset = reset_at >= block_len

    at_row = lax.broadcasted_iota(jnp.int32, (block_len, block_len), 0)
    at_col = lax.broadcasted_iota(jnp.int32, (block_len, block_len), 1)
    loads["dt"].wait()
    elapsed = jnp.dot(
        dt_ref[...], (at_row <= at_col).astype(F32),
        precision=lax.Precision.HIGHEST, preferred_element_type=F32,
    )
    for h in range(head_count):
        q, k = divmod(h, per)
        rows[q, k : k + 1, :] = elapsed[h : h + 1]
        rows[q, per + k : per + k + 1, :] = dt_ref[h : h + 1, :]
    loads["c"].wait()
    ct[...] = c_ref[...].T
    lane_of = lax.broadcasted_iota(jnp.int32, (1, LANES), 1)

    def spread(items):
        out = items[0]
        for k in range(1, per):
            out = jnp.where(lane_of >= k * width, items[k], out)
        return out

    def columns(j):
        return rows[j].T

    def at(j):
        return pl.ds(pl.multiple_of(j * LANES, LANES), LANES)

    def lanes(cols, kind):
        return spread([cols[:, kind * per + k : kind * per + k + 1] for k in range(per)])

    part = states // PIECES

    def span(p):
        begin = GAIN_ROWS + p * part if p else 0
        return pl.ds(begin, GAIN_ROWS + (p + 1) * part - begin)

    def of(p):
        return pl.ds(p * part, part)

    def copy_a(jj, p):
        return pltpu.make_async_remote_copy(
            src_ref=bg.at[(1 - side) * half + jj, span(p)], dst_ref=rxa.at[jj, span(p)],
            send_sem=a_send.at[jj, p], recv_sem=a_recv.at[jj, p],
            device_id={"seq": partner}, device_id_type=MESH,
        )

    def copy_e(jj, p):
        return pltpu.make_async_remote_copy(
            src_ref=ebuf.at[jj, of(p)], dst_ref=rxe.at[jj, of(p)],
            send_sem=e_send.at[jj, p], recv_sem=e_recv.at[jj, p],
            device_id={"seq": below}, device_id_type=MESH,
        )

    def copy_r(jj, p, holder):
        return pltpu.make_async_remote_copy(
            src_ref=ret.at[jj, of(p)], dst_ref=car.at[holder * half + jj, of(p)],
            send_sem=r_send.at[jj, p], recv_sem=r_recv.at[jj, p],
            device_id={"seq": partner}, device_id_type=MESH,
        )

    def boundary(j):
        now = rows[j]
        row_of = lax.broadcasted_iota(jnp.int32, (per, block_len), 0)
        token = lax.broadcasted_iota(jnp.int32, (per, block_len), 1)
        later = token >= reset_at
        decay = jnp.full((per, block_len), dec_ref[j * per], F32)
        for k in range(1, per):
            decay = jnp.where(row_of == k, dec_ref[j * per + k], decay)
        log_decay = -decay * now[0:per]
        final = log_decay[:, block_len - 1 : block_len]
        rows[j, 2 * per : 3 * per, :] = jnp.where(later, 0.0, jnp.exp(log_decay))
        rows[j, 3 * per : 4 * per, :] = jnp.where(later | no_reset, jnp.exp(final - log_decay), 0.0)
        gain = jnp.where(no_reset, jnp.exp(final), 0.0)
        cols = columns(j)
        weighted = g_ref[:, at(j)].astype(F32) * lanes(cols, 2)
        high, low = split(weighted)
        bg[j, GAIN_ROWS : GAIN_ROWS + states, :] = dot(ct[...], high) + dot(ct[...], low)
        gain_row = spread([gain[k : k + 1, :] for k in range(per)])
        bg[j, 0:GAIN_ROWS, :] = jnp.broadcast_to(gain_row, (GAIN_ROWS, LANES))

    loads["g"].wait()
    boundary((1 - side) * half)
    pl.semaphore_wait(barrier, n + nh - 2)

    def give(jj, _):
        boundary((1 - side) * half + jj)
        for p in range(PIECES):
            copy_a(jj - 1, p).start()
        return 0

    lax.fori_loop(1, half, give, 0)
    boundary(side * half)
    for p in range(PIECES):
        copy_a(half - 1, p).start()

    def keep(jj, _):
        boundary(side * half + jj)
        return 0

    lax.fori_loop(1, half, keep, 0)

    loads["b"].wait()
    joined = ((at_row >= reset_at) == (at_col >= reset_at)) & (at_col >= at_row)
    inter[...] = jnp.where(joined, dot_nt(b_ref[...], c_ref[...]), 0.0)
    acc[...] = jnp.zeros_like(acc)
    gbs[...] = jnp.zeros_like(gbs)

    @pl.when(last_group)
    def _():
        rxe[...] = jnp.zeros_like(rxe)

    loads["x"].wait()
    loads["s"].wait()

    def relay(jj):
        j = side * half + jj
        for p in range(PIECES):
            copy_a(jj, p).wait_recv()

            @pl.when(jnp.logical_not(last_group))
            def _():
                copy_e(jj, p).wait_recv()

            if p == 0:
                own_gain = bg[j, 0:1, :]
                other_gain = rxa[jj, 0:1, :]
                early_gain = jnp.where(first_side, own_gain, other_gain)
                late_gain = jnp.where(first_side, other_gain, own_gain)
            here = pl.ds(GAIN_ROWS + p * part, part)
            own = bg[j, here, :]
            other = rxa[jj, here, :]
            early = jnp.where(first_side, own, other)
            late = jnp.where(first_side, other, own)
            ending = rxe[jj, of(p), :]
            first = late + late_gain * ending

            @pl.when(group > 0)
            def _():
                ebuf[jj, of(p), :] = early + early_gain * first

            car[j, of(p), :] = jnp.where(first_side, first, ending)
            ret[jj, of(p), :] = jnp.where(first_side, ending, first)

            @pl.when(group > 0)
            def _():
                copy_e(jj, p).start()

            copy_r(jj, p, side).start()

    def pairs(j):
        now = rows[j]
        cols = columns(j)
        x_two = x_ref[:, at(j)]
        g_two = g_ref[:, at(j)]
        low_g = g_two[half_len:]
        inner = []
        terms = []
        for k in range(per):
            mine = (lane_of >= k * width) & (lane_of < (k + 1) * width)
            x_one = jnp.where(mine, x_two, jnp.zeros_like(x_two))
            rate_of = -dec_ref[j * per + k]
            parts = []
            total = jnp.zeros((1, LANES), F32)
            for top, left in ((0, 0), (half_len, half_len)):
                s_of = slice(top, top + half_len)
                u_of = slice(left, block_len)
                grad = g_two if left == 0 else low_g
                products = dot_nt(x_one[s_of], grad)
                gaps = now[k : k + 1, u_of] - cols[s_of, k : k + 1]
                gaps = jnp.maximum(gaps, 0.0)
                weight = jnp.exp(gaps * rate_of)
                mixing = weight * inter[s_of, u_of]
                scaled = weight * products * cols[s_of, per + k : per + k + 1]
                acc[s_of, u_of] += scaled
                parts.append(dot(mixing.astype(BF16), grad))
                inside = jnp.sum(mixing * gaps * products * cols[s_of, per + k : per + k + 1], axis=0, keepdims=True)
                for piece in range(0, inside.shape[1], LANES):
                    total = total + inside[:, piece : piece + LANES]
            inner.append(jnp.concatenate(parts, axis=0))
            shifted = total
            for k2 in range(1, per):
                shifted = shifted + pltpu.roll(total, k2 * width, 1)
            terms.append(shifted)
        dxi[j] = spread(inner)
        inside_row = spread(terms)
        state = s_ref[pl.ds(j * per, per)].reshape(LANES, states).T
        st[j] = state
        high, low = split(state)
        read = dot(c_ref[...], high) + dot(c_ref[...], low)
        entry = g_two.astype(F32) * read * (lanes(cols, 2) * lanes(cols, 0))
        entry_row = jnp.sum(entry, axis=0, keepdims=True)
        rate[j] = jnp.broadcast_to(inside_row + entry_row, (8, LANES))

    def finish(j):
        cols = columns(j)
        carried = car[j]
        high, low = split(carried)
        through = jnp.sum(carried * st[j], axis=0, keepdims=True)
        step = lanes(cols, 1)
        end = lanes(cols, 3)
        spent = lanes(cols, 0)
        last = spent[block_len - 1 : block_len]
        reach = end * (dot(b_ref[...], high) + dot(b_ref[...], low))
        gx_ref[:, at(j)] = (step * (dxi[j] + reach)).astype(BF16)
        x_step = x_ref[:, at(j)].astype(F32) * step
        leaving = jnp.sum(x_step * reach * (last - spent), axis=0, keepdims=True)
        x_high, x_low = split(x_step * end)
        gbs[...] += dot_nt(x_high, high) + dot_nt(x_high, low) + dot_nt(x_low, high)
        gain_row = bg[j, 0:1, :]
        rate[j] += jnp.broadcast_to(leaving + gain_row * last * through, (8, LANES))

    base = max(chunks - 1, (groups - 1) * LAG)
    lag = base - group * LAG

    def slot(t, _):
        jj = t - lag

        @pl.when((jj >= 0) & (jj < half))
        def _():
            relay(jj)

        @pl.when(t < chunks)
        def _():
            pairs(t)

        @pl.when((t >= base) & (t < base + half))
        def _():
            finish(side * half + t - base)

        late = t - base - 2

        @pl.when(late >= 0)
        def _():
            for p in range(PIECES):
                copy_r(late, p, 1 - side).wait_recv()
            finish((1 - side) * half + late)

        return 0

    lax.fori_loop(0, base + half, slot, 0)
    summed = jnp.where(joined, acc[...], 0.0)
    sum_high, sum_low = split(summed)
    gbs[...] += dot(sum_high, c_ref[...]) + dot(sum_low, c_ref[...])
    lax.fori_loop(base + half, base + half + 2, slot, 0)

    share = block_len // nh

    def copy_g(d):
        peer = lax.rem(me_h + d, nh)
        return pltpu.make_async_remote_copy(
            src_ref=gbs.at[pl.ds(pl.multiple_of(peer * share, share), share)], dst_ref=rxg.at[d],
            send_sem=g_send.at[d], recv_sem=g_recv.at[d],
            device_id={"head": peer}, device_id_type=MESH,
        )

    def copy_f(d):
        peer = lax.rem(me_h + d, nh)
        return pltpu.make_async_remote_copy(
            src_ref=gsum, dst_ref=gfin.at[d],
            send_sem=f_send.at[d], recv_sem=f_recv.at[d],
            device_id={"head": peer}, device_id_type=MESH,
        )

    def copy_t(d):
        return pltpu.make_async_remote_copy(
            src_ref=rtot, dst_ref=rxr.at[d],
            send_sem=t_send.at[d], recv_sem=t_recv.at[d],
            device_id={"seq": lax.rem(me + d, n)}, device_id_type=MESH,
        )

    for d in range(1, nh):
        copy_g(d).start()

    parity = lax.broadcasted_iota(jnp.int32, (LANES, LANES), 0) // width
    target = lax.broadcasted_iota(jnp.int32, (LANES, LANES), 1)
    chosen = (lax.rem(target, per) == parity).astype(F32)
    folded = jnp.concatenate([rate[j, 0:1, :] for j in range(chunks)], axis=0)
    sums = jnp.dot(folded, chosen, precision=lax.Precision.HIGHEST, preferred_element_type=F32)
    home = lax.broadcasted_iota(jnp.int32, (chunks, LANES), 1) // per
    which = lax.broadcasted_iota(jnp.int32, (chunks, LANES), 0)
    mine_rate = jnp.sum(jnp.where(home == which, sums, 0.0), axis=0, keepdims=True)
    rtot[...] = jnp.broadcast_to(mine_rate, (8, LANES))

    own_share = gbs[pl.ds(pl.multiple_of(me_h * share, share), share), :]
    for d in range(1, n):
        copy_t(d).start()
    for d in range(1, nh):
        copy_g(d).wait_recv()
        own_share = own_share + rxg[d]
    gsum[...] = own_share
    gb_ref[pl.ds(pl.multiple_of(me_h * share, share), share), :] = own_share
    for d in range(1, nh):
        copy_f(d).start()
    all_rate = rtot[...]
    for d in range(1, n):
        copy_t(d).wait_recv()
        all_rate = all_rate + rxr[d]
    rate_ref[...] = -all_rate
    for d in range(1, nh):
        copy_f(d).wait_recv()
        source = lax.rem(me_h + nh - d, nh)
        gb_ref[pl.ds(pl.multiple_of(source * share, share), share), :] = gfin[d]

    for jj in range(half):
        for p in range(PIECES):
            copy_a(jj, p).wait_send()
            copy_r(jj, p, side).wait_send()

    @pl.when(group > 0)
    def _():
        for jj in range(half):
            for p in range(PIECES):
                copy_e(jj, p).wait_send()

    for d in range(1, nh):
        copy_g(d).wait_send()
        copy_f(d).wait_send()
    for d in range(1, n):
        copy_t(d).wait_send()


def body(n, nh, inputs, time_step, decay_rate, input_map, output_map, output_grad, span_states, resets):
    head_count, block_len = time_step.shape
    width, states = span_states.shape[2:]
    chunks = inputs.shape[1] // LANES
    half = chunks // 2
    share = block_len // nh
    vmem = pl.BlockSpec(memory_space=pltpu.VMEM)
    hbm = pl.BlockSpec(memory_space=pltpu.HBM)
    sem = pltpu.SemaphoreType.DMA
    state = span_states.reshape(span_states.shape[1:])
    operands = [
        pltpu.with_memory_space_constraint(operand, pltpu.HBM)
        for operand in (inputs, output_grad, time_step, decay_rate, input_map, output_map, state)
    ]
    grad_inputs, grad_map, rates = pl.pallas_call(
        functools.partial(kernel, n, nh, width),
        out_shape=(
            jax.ShapeDtypeStruct(inputs.shape, BF16),
            jax.ShapeDtypeStruct((block_len, states), F32),
            jax.ShapeDtypeStruct((8, LANES), F32),
        ),
        in_specs=[hbm] * 8,
        out_specs=(vmem, vmem, vmem),
        scratch_shapes=[
            pltpu.VMEM(inputs.shape, BF16),
            pltpu.VMEM(inputs.shape, BF16),
            pltpu.VMEM(time_step.shape, F32),
            pltpu.SMEM(decay_rate.shape, F32),
            pltpu.VMEM(input_map.shape, BF16),
            pltpu.VMEM(output_map.shape, BF16),
            pltpu.VMEM(span_states.shape[1:], F32),
            pltpu.SMEM(resets.shape, jnp.int32),
            sem((8,)),
            pltpu.VMEM((chunks, 8, block_len), F32),
            pltpu.VMEM((states, block_len), BF16),
            pltpu.VMEM((block_len, block_len), F32),
            pltpu.VMEM((block_len, block_len), F32),
            pltpu.VMEM((chunks, states, LANES), F32),
            pltpu.VMEM((chunks, block_len, LANES), F32),
            pltpu.VMEM((chunks, 8, LANES), F32),
            pltpu.VMEM((chunks, states + GAIN_ROWS, LANES), F32),
            pltpu.VMEM((half, states + GAIN_ROWS, LANES), F32),
            pltpu.VMEM((half, states, LANES), F32),
            pltpu.VMEM((half, states, LANES), F32),
            pltpu.VMEM((half, states, LANES), F32),
            pltpu.VMEM((chunks, states, LANES), F32),
            pltpu.VMEM((block_len, states), F32),
            pltpu.VMEM((nh, share, states), F32),
            pltpu.VMEM((share, states), F32),
            pltpu.VMEM((nh, share, states), F32),
            pltpu.VMEM((8, LANES), F32),
            pltpu.VMEM((n, 8, LANES), F32),
            *[sem((half, PIECES)) for _ in range(6)],
            sem((nh,)), sem((nh,)), sem((nh,)), sem((nh,)), sem((n,)), sem((n,)),
        ],
        compiler_params=pltpu.CompilerParams(
            collective_id=0, has_side_effects=True, vmem_limit_bytes=40 * 2**20
        ),
    )(*operands, resets)
    return grad_inputs, grad_map, rates[0, :head_count]


def solution(mesh):
    in_specs = (
        P("seq", "head"),
        P("head", "seq"),
        P("head"),
        P("seq", None),
        P("seq", None),
        P("seq", "head"),
        P("seq", "head", None, None),
        P("seq"),
    )
    out_specs = (P("seq", "head"), P("seq", None), P("head"))
    run = functools.partial(body, mesh.shape["seq"], mesh.shape["head"])
    return jax.shard_map(run, mesh=mesh, in_specs=in_specs, out_specs=out_specs, check_vma=False)
```
